256 devices in a mesh: section: 8 (over z_lo, core), dp: 8 (over y, z_hi), tensor: 4 (over x).
Axes of the slice: x: 4, y: 4, z: 8 (z_hi: 2, z_lo: 4; z = z_hi * 4 + z_lo), core: 2. Of those that a mesh axis runs over, the one named last changes fastest.
Arguments:
- inputs: bfloat16 [32, 2, 64, 2560], P('dp', None, None, ('section', 'tensor')), parts along dimension 0, may hold values from -18 to 18
- sequence_jobs: int32 [32, 2, 1], P('dp'), parts along dimension 0, may hold values from 0 to 3
- entry_sequence: int32 [32], P('dp'), parts along dimension 0, may hold values from 0 to 3, each once
- layer_norm_gain: float32 [8, 2560], P('section'), may hold values from 0.25 to 1.75
- frozen_query_matrix: bfloat16 [8, 2560, 2560], P('section', None, 'tensor'), may hold values from -1 to 1
- frozen_key_matrix: bfloat16 [8, 2560, 2560], P('section', None, 'tensor'), may hold values from -24 to 24
- frozen_value_matrix: bfloat16 [8, 2560, 2560], P('section', None, 'tensor'), may hold values from -0.125 to 0.125
- frozen_output_matrix: bfloat16 [8, 2560, 2560], P('section', 'tensor'), may hold values from -0.125 to 0.125
- adapter_down_maps: bfloat16 [8, 2560, 128], P('section', 'tensor'), may hold values from -0.125 to 0.125
- adapter_up_maps: bfloat16 [8, 2, 64, 2560], P('section', None, None, 'tensor'), may hold values from -1.5 to 1.5
Outputs:
- finished: bfloat16 [32, 2, 64, 2560], P('dp', None, None, ('section', 'tensor')), parts along dimension 0
The draws below stay inside these ranges and needn't reach their ends.
There are 8 independent parts, one for each index of `dp`. The reference program is written for one: setup_inputs(seed, part) draws one part's arguments, and reference() takes and returns one part's arrays. A program takes and returns all parts, laid end to end along the dimension named above; an argument that names none is the same for every part. Nothing has to cross between parts.
Inputs may be any that keep to these rules, and one draw needn't show every extreme that they name: `sequence_jobs`: every one of the 4 jobs owns at least one sequence. `entry_sequence`: a permutation of the 4 micro-batches.
All inputs are finite; a program needn't handle non-finite values.
Results may differ from the reference program's by a relative error of at most 0.039.
Values may be sent and summed in bfloat16 or wider, within the bound.
No kernel may reach another device: no remote copies, remote signals or barrier semaphores. Data moves between devices by JAX's collectives and lax.ppermute only.
A program may use at most 64 MiB of HBM per device.

```python
import math
import jax
import jax.numpy as jnp
from jax import lax

MODEL_WIDTH = 2560
HEADS = 20
HEAD_DIM = 128
ADAPTER_RANK = 16
ADAPTER_JOBS = 4
MICRO_SEQUENCES = 2
SEQ = 64
MICRO_BATCHES = 4
WINDOW_LAYERS = 8
N_TENSOR = 4


def shared_projection(key):
    base = jax.random.normal(jax.random.fold_in(key, 11), (WINDOW_LAYERS, MODEL_WIDTH, HEADS * HEAD_DIM), jnp.float32)
    return jnp.clip(base, -6.0, 6.0) / math.sqrt(MODEL_WIDTH)


def draw_frozen_query_matrix(key, part):
    return shared_projection(key).astype(jnp.bfloat16)


def draw_frozen_key_matrix(key, part):
    own_part = jax.random.normal(jax.random.fold_in(key, 12), (WINDOW_LAYERS, MODEL_WIDTH, HEADS * HEAD_DIM), jnp.float32)
    own_part = jnp.clip(own_part, -6.0, 6.0) / math.sqrt(MODEL_WIDTH)
    return own_part.astype(jnp.bfloat16)


def draw_inputs(key, part):
    full_shape = (MICRO_BATCHES, MICRO_SEQUENCES, SEQ, MODEL_WIDTH)
    base = jax.random.normal(jax.random.fold_in(key, 21), full_shape, jnp.float32)
    return jnp.clip(base, -6.0, 6.0).astype(jnp.bfloat16)


def block_levels(own_key, shape, split, least, high):
    def one(position, shards_of):
        draws = jax.random.uniform(jax.random.fold_in(jax.random.fold_in(own_key, 6), position), (shards_of,), jnp.float32, least / len(split), high / len(split))
        return jnp.repeat(jnp.exp(draws), shape[position] // shards_of).reshape((-1,) + (1,) * (len(shape) - position - 1))

    factor_of = one(*split[0])
    for cut in split[1:]:
        factor_of = factor_of * one(*cut)
    return factor_of


def different_ones(key, rows, number_of, top, lift):
    ranking = jax.random.permutation(jax.random.fold_in(key, 1), number_of)
    pull = ranking
    for power in range(3):
        pull = pull * pull // number_of
    pull = pull * lift // number_of
    tickets = jax.random.randint(jax.random.fold_in(key, 2), (rows, number_of), 0, 4096) + pull
    holders = jax.random.permutation(jax.random.fold_in(key, 3), rows)[jnp.arange(number_of) % rows]
    tickets = jnp.where(jnp.arange(rows)[:, None] == holders[None, :], 1 << 14, tickets)
    priority = tickets * number_of + jnp.arange(number_of)
    return lax.top_k(priority.astype(jnp.int32), top)[1].astype(jnp.int32)


def centred(rng, dims, scale, reach, pieces=(), held_as=jnp.bfloat16):
    factor_of = block_levels(rng, dims, pieces, -0.22, 0.18) if pieces else 1.0
    values = jax.random.normal(rng, dims, jnp.float32) * scale * factor_of
    return jnp.minimum(jnp.maximum(values, -reach), reach).astype(held_as)


def setup_inputs(seed: int = 0, part: int = 0) -> dict:
    seeds = jax.random.split(jax.random.key(seed), 11)
    own_keys = jax.random.split(jax.random.fold_in(seeds[10], part), 11)
    return {
        "inputs": draw_inputs(jax.random.fold_in(jax.random.fold_in(seeds[10], part), 71), part),
        "sequence_jobs": different_ones(own_keys[1], MICRO_BATCHES * MICRO_SEQUENCES, ADAPTER_JOBS, 1, 2048).reshape((MICRO_BATCHES, MICRO_SEQUENCES, 1)),
        "entry_sequence": jax.random.permutation(own_keys[2], MICRO_BATCHES).astype(jnp.int32),
        "layer_norm_gain": jnp.clip(1.0 + 0.15 * jax.random.normal(seeds[3], (WINDOW_LAYERS, MODEL_WIDTH), jnp.float32), 0.25, 1.75),
        "frozen_query_matrix": draw_frozen_query_matrix(jax.random.fold_in(seeds[10], 71), part),
        "frozen_key_matrix": draw_frozen_key_matrix(jax.random.fold_in(seeds[10], 71), part),
        "frozen_value_matrix": centred(seeds[6], (WINDOW_LAYERS, MODEL_WIDTH, MODEL_WIDTH), MODEL_WIDTH ** -0.5, 0.125, ((0, 8), (2, 4))),
        "frozen_output_matrix": centred(seeds[7], (WINDOW_LAYERS, MODEL_WIDTH, MODEL_WIDTH), MODEL_WIDTH ** -0.5, 0.125, ((0, 8), (1, 4))),
        "adapter_down_maps": centred(seeds[8], (WINDOW_LAYERS, MODEL_WIDTH, 2 * ADAPTER_JOBS * ADAPTER_RANK), MODEL_WIDTH ** -0.5, 0.125, ((0, 8), (1, 4))),
        "adapter_up_maps": centred(seeds[9], (WINDOW_LAYERS, 2, ADAPTER_JOBS * ADAPTER_RANK, MODEL_WIDTH), ADAPTER_RANK ** -0.5, 1.5, ((0, 8), (3, 4))),
    }


adapter_scale = 2.0

def attend(query_rows, key_vecs, value_rows, head_groupings):
    head_count = query_rows.shape[1] // HEAD_DIM
    grid_shape = (head_groupings, SEQ, head_count, HEAD_DIM)
    q_wide = query_rows.reshape(grid_shape).astype(jnp.float32)
    k_wide = key_vecs.reshape(grid_shape).astype(jnp.float32)
    v_wide = value_rows.reshape(grid_shape).astype(jnp.float32)
    scores = jnp.einsum('bqhd,bkhd->bhqk', q_wide, k_wide) * HEAD_DIM ** (-0.5)
    causal = jnp.arange(SEQ, dtype=jnp.int32)[:, None] >= jnp.arange(SEQ, dtype=jnp.int32)[None, :]
    scores = jnp.where(causal, scores, -jnp.inf)
    row_max = lax.optimization_barrier(jnp.max(scores, axis=-1, keepdims=True))
    weights = jnp.exp(scores - row_max)
    probabilities = (weights / lax.optimization_barrier(jnp.sum(weights, axis=-1, keepdims=True))).astype(jnp.bfloat16)
    mixture = jnp.einsum('bhqk,bkhd->bqhd', probabilities.astype(jnp.float32), v_wide)
    return mixture.astype(jnp.bfloat16).reshape(head_groupings * SEQ, head_count * HEAD_DIM)

def layer_forward(hidden_state, job_per_row, inverse_norm_scale, query_matrix, key_matrix, value_matrix, output_matrix, adapter_lower_part, adapter_upper_part, head_groupings):
    widened = hidden_state.astype(jnp.float32)
    meansq = lax.optimization_barrier(jnp.mean(widened * widened, axis=-1, keepdims=True))
    normalized_input = (widened * lax.rsqrt(meansq + 1e-05) * inverse_norm_scale).astype(jnp.bfloat16)
    lowrank_products = jnp.dot(normalized_input, adapter_lower_part, preferred_element_type=jnp.float32)
    column_job = jnp.arange(lowrank_products.shape[1], dtype=jnp.int32) // ADAPTER_RANK % ADAPTER_JOBS
    lowrank_products = jnp.where(column_job[None, :] == job_per_row[:, None], lowrank_products, 0.0).astype(jnp.bfloat16)
    middle_result = lowrank_products.shape[1] // 2
    query_rows = (jnp.dot(normalized_input, query_matrix, preferred_element_type=jnp.float32) + adapter_scale * jnp.dot(lowrank_products[:, :middle_result], adapter_upper_part[0], preferred_element_type=jnp.float32)).astype(jnp.bfloat16)
    key_vecs = jnp.dot(normalized_input, key_matrix, preferred_element_type=jnp.float32).astype(jnp.bfloat16)
    value_rows = (jnp.dot(normalized_input, value_matrix, preferred_element_type=jnp.float32) + adapter_scale * jnp.dot(lowrank_products[:, middle_result:], adapter_upper_part[1], preferred_element_type=jnp.float32)).astype(jnp.bfloat16)
    heads = attend(query_rows, key_vecs, value_rows, head_groupings)
    rows = heads.shape[0]
    block = MODEL_WIDTH // N_TENSOR
    head_blocks = heads.reshape(rows, N_TENSOR, block).astype(jnp.float32)
    weight_blocks = output_matrix.reshape(N_TENSOR, block, MODEL_WIDTH).astype(jnp.float32)
    partial_value = jnp.einsum('rbf,bfe->bre', head_blocks, weight_blocks).astype(jnp.bfloat16)
    partial_value = lax.optimization_barrier(partial_value)
    summed = lax.optimization_barrier(jnp.sum(partial_value.astype(jnp.float32), axis=0))
    return (widened + summed).astype(jnp.bfloat16)

def reference(inputs, sequence_jobs, entry_sequence, layer_norm_gain, frozen_query_matrix, frozen_key_matrix, frozen_value_matrix, frozen_output_matrix, adapter_down_maps, adapter_up_maps):
    ordered = jnp.take(inputs, entry_sequence, axis=0)
    seq_jobs = jnp.take(sequence_jobs, entry_sequence, axis=0)[:, :, 0]
    job_per_row = jnp.repeat(seq_jobs.reshape(-1), SEQ)
    hidden_state = ordered.reshape(MICRO_BATCHES * MICRO_SEQUENCES * SEQ, MODEL_WIDTH)
    for layer_number in range(WINDOW_LAYERS):
        hidden_state = layer_forward(hidden_state, job_per_row, layer_norm_gain[layer_number], frozen_query_matrix[layer_number], frozen_key_matrix[layer_number], frozen_value_matrix[layer_number], frozen_output_matrix[layer_number], adapter_down_maps[layer_number], adapter_up_maps[layer_number], MICRO_BATCHES * MICRO_SEQUENCES)
    return hidden_state.reshape(MICRO_BATCHES, MICRO_SEQUENCES, SEQ, MODEL_WIDTH)
```

```python
import functools

import jax
import jax.numpy as jnp
from jax import lax
from jax.experimental import pallas as pl
from jax.experimental.pallas import tpu as pltpu
from jax.sharding import PartitionSpec as P

HEAD_DIM = 128
ADAPTER_RANK = 16
ADAPTER_JOBS = 4
SCALE = 2.0
EPS = 1e-05
BF = jnp.bfloat16
F32 = jnp.float32


def dot(a, b):
    return jnp.dot(a, b, preferred_element_type=F32)


def layer_kernel(meta, mask, x0, x1, x2, x3, *refs):
    own = refs[0:7]
    other = refs[7:14]
    ys = refs[14:18]
    frozen, down, up, gain, normed, total, heads, sems = refs[18:]
    xs = (x0, x1, x2, x3)
    tile = x0.shape[1]
    blocks = len(xs)
    rows = x0.shape[0]
    part = meta[0]
    choice = meta[1]

    def span(i, sign):
        block = lax.rem(part + blocks + sign * i, blocks)
        return pl.ds(pl.multiple_of(block * tile, tile), tile)

    def start(source):
        sq, sk, sv, so, sd, su, sg = source
        pltpu.make_async_copy(sg, gain, sems.at[4, 0]).start()
        pltpu.make_async_copy(sd, down, sems.at[4, 1]).start()
        pltpu.make_async_copy(su, up, sems.at[4, 2]).start()
        for i in range(blocks):
            for n, s in enumerate((sq, sk, sv)):
                pltpu.make_async_copy(s.at[span(i, -1)], frozen.at[n, i], sems.at[n, i]).start()
        for i in range(blocks):
            pltpu.make_async_copy(so.at[:, span(i, 1)], frozen.at[3, i], sems.at[3, i]).start()

    @pl.when(choice == 0)
    def _():
        start(own)

    @pl.when(choice != 0)
    def _():
        start(other)

    def ready(n, i):
        pltpu.make_async_copy(frozen.at[n, i], frozen.at[n, i], sems.at[n, i]).wait()

    wide = [x[...].astype(F32) for x in xs]
    square = sum(jnp.sum(w * w, axis=-1, keepdims=True) for w in wide)
    norm = lax.rsqrt(square * (1.0 / (tile * blocks)) + EPS)
    pltpu.make_async_copy(own[6], gain, sems.at[4, 0]).wait()
    pltpu.make_async_copy(own[4], down, sems.at[4, 1]).wait()
    codes = None
    for i in range(blocks):
        block = (wide[i] * norm * gain[lax.rem(part + (blocks - i), blocks)]).astype(BF)
        normed[i] = block
        code = dot(block, down[i])
        codes = code if codes is None else codes + code
    codes = (codes * mask[...]).astype(BF)
    half = codes.shape[1] // 2
    pltpu.make_async_copy(own[5], up, sems.at[4, 2]).wait()
    total[0] = SCALE * dot(codes[:, :half], up[0])
    total[1] = jnp.zeros((rows, tile), F32)
    total[2] = SCALE * dot(codes[:, half:], up[1])

    @pl.loop(0, blocks)
    def _(i):
        for n in range(3):
            ready(n, i)
            total[n] += dot(normed[i], frozen[n, i])

    query, keys, values = (total[n].astype(BF) for n in range(3))
    causal = lax.broadcasted_iota(jnp.int32, (rows, rows), 0) >= lax.broadcasted_iota(
        jnp.int32, (rows, rows), 1
    )
    for h in range(tile // HEAD_DIM):
        c = slice(h * HEAD_DIM, (h + 1) * HEAD_DIM)
        scores = lax.dot_general(
            query[:, c], keys[:, c], (((1,), (1,)), ((), ())), preferred_element_type=F32
        ) * (HEAD_DIM**-0.5)
        scores = jnp.where(causal, scores, -jnp.inf)
        weights = jnp.exp(scores - jnp.max(scores, axis=-1, keepdims=True))
        probs = (weights / jnp.sum(weights, axis=-1, keepdims=True)).astype(BF)
        heads[:, c] = dot(probs, values[:, c]).astype(BF)
    total[0] = x0[...].astype(F32)
    for i in range(1, blocks):
        total[i] = jnp.zeros((rows, tile), F32)

    @pl.loop(0, blocks // 2)
    def _(pair):
        for k in range(2):
            i = pair * 2 + k
            ready(3, i)
            total[i] += dot(heads[...], frozen[3, i])

    ys[0][...] = total[0]
    for i in range(1, blocks):
        ys[i][...] = total[i].astype(BF)


def layer(meta, mask, xs, own, other):
    rows, tile = xs[0].shape
    blocks = len(xs)
    vmem = pl.BlockSpec(memory_space=pltpu.VMEM)
    hbm = pl.BlockSpec(memory_space=pltpu.HBM)
    macs = rows * tile * tile * blocks * 4
    return pl.pallas_call(
        layer_kernel,
        out_shape=[
            jax.ShapeDtypeStruct((rows, tile), F32 if i == 0 else BF) for i in range(blocks)
        ],
        in_specs=[pl.BlockSpec(memory_space=pltpu.SMEM), vmem]
        + [vmem] * blocks
        + [hbm] * 14,
        out_specs=[vmem] * blocks,
        scratch_shapes=[
            pltpu.VMEM((4, blocks, tile, tile), BF),
            pltpu.VMEM(own[4].shape, BF),
            pltpu.VMEM(own[5].shape, BF),
            pltpu.VMEM(own[6].shape, F32),
            pltpu.VMEM((blocks, rows, tile), BF),
            pltpu.VMEM((blocks, rows, tile), F32),
            pltpu.VMEM((rows, tile), BF),
            pltpu.SemaphoreType.DMA((5, blocks)),
        ],
        cost_estimate=pl.CostEstimate(
            flops=4 * macs, bytes_accessed=8 * tile * tile * blocks, transcendentals=0
        ),
        compiler_params=pltpu.CompilerParams(vmem_limit_bytes=24 * 1024 * 1024),
        name="layer",
    )(meta, mask, *xs, *own, *other)


def shards(
    inputs,
    sequence_jobs,
    entry_sequence,
    layer_norm_gain,
    frozen_query_matrix,
    frozen_key_matrix,
    frozen_value_matrix,
    frozen_output_matrix,
    adapter_down_maps,
    adapter_up_maps,
):
    sections = lax.axis_size("section")
    across = lax.axis_size("tensor")
    stages = sections // 2
    section_id = lax.axis_index("section")
    part = lax.axis_index("tensor")
    core = section_id % 2
    stage = section_id // 2
    batches, _, length, piece = inputs.shape
    tile = frozen_query_matrix.shape[2]
    streams = 2
    chunks = batches // streams
    both = ("section", "tensor")

    def turned(value, step):
        return lax.ppermute(
            value, "tensor", [(i, (i + step) % across) for i in range(across)]
        )

    def swapped(value):
        return lax.ppermute(value, "section", [(i, i ^ 1) for i in range(sections)])

    def onward(value):
        return lax.ppermute(value, "section", [(i, i + 2) for i in range(sections - 2)])

    def tokens(which):
        return jnp.concatenate(
            [
                lax.dynamic_slice(
                    inputs, (entry_sequence[m], which, 0, 0), (1, 1, length, piece)
                ).reshape(1, length, piece)
                for m in range(batches)
            ],
            axis=0,
        )

    same_tokens, cross_tokens = tokens(core), tokens(1 - core)

    def collected(value, flip):
        return jnp.concatenate(
            [
                lax.ppermute(
                    value,
                    both,
                    [
                        ((2 * j + e) * across + r, (e ^ flip) * across + j)
                        for j in range(stages)
                        for e in range(2)
                    ],
                )
                for r in range(across)
            ],
            axis=2,
        )

    same_half, cross_half = collected(same_tokens, 0), collected(cross_tokens, 1)
    entering = jnp.where(
        core == 0,
        jnp.concatenate([same_half, cross_half], axis=2),
        jnp.concatenate([cross_half, same_half], axis=2),
    )

    down_own = adapter_down_maps[0]
    down_all = jnp.stack([down_own] + [turned(down_own, d) for d in range(1, across)])
    own = (
        frozen_query_matrix[0],
        frozen_key_matrix[0],
        frozen_value_matrix[0],
        frozen_output_matrix[0],
        down_all,
        adapter_up_maps[0],
        layer_norm_gain.reshape(across, 1, tile),
    )
    other = tuple(swapped(w) for w in own)
    metas = [
        jnp.stack([part, core if l == 0 else 1 - core]).astype(jnp.int32) for l in range(2)
    ]
    column_job = (
        lax.broadcasted_iota(jnp.int32, (1, adapter_down_maps.shape[2]), 1)
        // ADAPTER_RANK
        % ADAPTER_JOBS
    )

    def mask_of(step, stream):
        m = jnp.clip((step - stage) * streams + stream, 0, batches - 1)
        job = lax.dynamic_slice(sequence_jobs, (entry_sequence[m], core, 0), (1, 1, 1))
        return (column_job == job.reshape(1, 1)).astype(F32)

    def gathered(x):
        return [x] + [turned(x, d) for d in range(1, across)]

    def scattered(ys):
        total = ys[0]
        for d in range(1, across):
            total = total + turned(ys[d], d).astype(F32)
        return total.astype(BF)

    def spread(block):
        first, second = block[..., : tile // 2], block[..., tile // 2 :]
        halves = (
            jnp.where(core == 0, first, second),
            jnp.where(core == 0, second, first),
        )
        found = []
        for flip in range(2):
            total = None
            for r in range(across):
                got = lax.ppermute(
                    halves[flip][..., r * piece : (r + 1) * piece],
                    both,
                    [
                        ((sections - 2 + e) * across + j, (2 * j + (e ^ flip)) * across + r)
                        for j in range(stages)
                        for e in range(2)
                    ],
                )
                total = got if total is None else total + got
            found.append(total)
        return jnp.where(
            core == 0, jnp.stack(found, axis=1), jnp.stack(found[::-1], axis=1)
        )

    carried = [None] * streams
    results = []
    for step in range(chunks + stages - 1):
        masks = [mask_of(step, s) for s in range(streams)]
        xs = []
        for s in range(streams):
            if step < chunks:
                fresh = entering[step * streams + s]
                x = fresh if step == 0 else jnp.where(stage == 0, fresh, carried[s])
            else:
                x = carried[s]
            xs.append(x)
        for l in range(2):
            for s in range(streams):
                ys = layer(metas[l], masks[s], gathered(xs[s]), own, other)
                xs[s] = scattered(ys)
        if step >= stages - 1:
            results.append(spread(jnp.stack(xs)))
        if step < chunks + stages - 2:
            carried = [onward(x) for x in xs]
    return jnp.concatenate(results, axis=0)


def solution(mesh):
    in_specs = (
        P("dp", None, None, ("section", "tensor")),
        P("dp", None, None),
        P("dp"),
        P("section", None),
        P("section", None, "tensor"),
        P("section", None, "tensor"),
        P("section", None, "tensor"),
        P("section", "tensor", None),
        P("section", "tensor", None),
        P("section", None, None, "tensor"),
    )
    out_specs = P("dp", None, None, ("section", "tensor"))
    return jax.shard_map(shards, mesh=mesh, in_specs=in_specs, out_specs=out_specs, check_vma=False)
```

```python
import functools

import jax
import jax.numpy as jnp
from jax import lax
from jax.experimental import pallas as pl
from jax.experimental.pallas import tpu as pltpu
from jax.sharding import PartitionSpec as P

HEAD_DIM = 128
ADAPTER_RANK = 16
ADAPTER_JOBS = 4
SCALE = 2.0
EPS = 1e-05
BF = jnp.bfloat16
F32 = jnp.float32


def dot(a, b):
    return jnp.dot(a, b, preferred_element_type=F32)


def load_kernel(choice, *refs):
    count = (len(refs) - 1) // 3
    own, other, out, sems = refs[:count], refs[count : 2 * count], refs[2 * count : -1], refs[-1]

    def start(source):
        for n in range(count):
            pltpu.make_async_copy(source[n], out[n], sems.at[n]).start()

    @pl.when(choice[0] == 0)
    def _():
        start(own)

    @pl.when(choice[0] != 0)
    def _():
        start(other)

    for n in range(count):
        pltpu.make_async_copy(own[n], out[n], sems.at[n]).wait()


def load(choice, own, other, limit):
    vmem = pl.BlockSpec(memory_space=pltpu.VMEM)
    hbm = pl.BlockSpec(memory_space=pltpu.HBM)
    count = len(own)
    return pl.pallas_call(
        load_kernel,
        out_shape=[jax.ShapeDtypeStruct(w.shape, w.dtype) for w in own],
        in_specs=[pl.BlockSpec(memory_space=pltpu.SMEM)] + [hbm] * (2 * count),
        out_specs=[vmem] * count,
        scratch_shapes=[pltpu.SemaphoreType.DMA((count,))],
        cost_estimate=pl.CostEstimate(
            flops=4 * 10**9, bytes_accessed=8 * own[0].size, transcendentals=0
        ),
        compiler_params=pltpu.CompilerParams(vmem_limit_bytes=limit * 1024 * 1024),
        name="load",
    )(choice, *own, *other)


def assemble_kernel(core, *refs):
    pieces, out = refs[:-1], refs[-1]
    count = len(pieces)
    width = pieces[0].shape[3]
    first = core[0] == 0
    for r, piece in enumerate(pieces):
        same, cross = piece[0], piece[1]
        out[:, :, r * width : (r + 1) * width] = jnp.where(first, same, cross)
        out[:, :, (count + r) * width : (count + r + 1) * width] = jnp.where(first, cross, same)


def assemble(core, pieces):
    halves, batches, length, width = pieces[0].shape
    vmem = pl.BlockSpec(memory_space=pltpu.VMEM)
    return pl.pallas_call(
        assemble_kernel,
        out_shape=jax.ShapeDtypeStruct((batches, length, width * halves * len(pieces)), BF),
        in_specs=[pl.BlockSpec(memory_space=pltpu.SMEM)] + [vmem] * len(pieces),
        out_specs=vmem,
        compiler_params=pltpu.CompilerParams(vmem_limit_bytes=8 * 1024 * 1024),
        name="assemble",
    )(core, *pieces)


def layer_kernel(
    length, first, meta, jobs, x0, x1, x2, x3, wq, wk, wv, wo, down, up, gain, y0, y1, y2, y3, normed, heads
):
    xs, ys = (x0, x1, x2, x3), (y0, y1, y2, y3)
    rows, tile = x0.shape
    blocks = len(xs)
    part = meta[0]
    sequences = rows // length
    column_job = (
        lax.broadcasted_iota(jnp.int32, (length, down.shape[2]), 1) // ADAPTER_RANK % ADAPTER_JOBS
    )
    own_job = jnp.concatenate(
        [(column_job == jobs[first + q]).astype(F32) for q in range(sequences)], axis=0
    )
    wide = [x[...].astype(F32) for x in xs]
    square = sum(jnp.sum(w * w, axis=-1, keepdims=True) for w in wide)
    norm = lax.rsqrt(square * (1.0 / (tile * blocks)) + EPS)
    codes = None
    for i in range(blocks):
        rank = lax.rem(part + (blocks - i), blocks)
        block = (wide[i] * norm * gain[rank]).astype(BF)
        normed[rank] = block
        code = dot(block, down[i])
        codes = code if codes is None else codes + code
    codes = jnp.where(own_job > 0.0, codes, 0.0).astype(BF)
    half = codes.shape[1] // 2

    def projected(w):
        total = None
        for i in range(blocks):
            product = dot(normed[i], w[i * tile : (i + 1) * tile])
            total = product if total is None else total + product
        return total

    query = (projected(wq) + SCALE * dot(codes[:, :half], up[0])).astype(BF)
    keys = projected(wk).astype(BF)
    values = (projected(wv) + SCALE * dot(codes[:, half:], up[1])).astype(BF)
    causal = lax.broadcasted_iota(jnp.int32, (length, length), 0) >= lax.broadcasted_iota(
        jnp.int32, (length, length), 1
    )
    spans = [
        (slice(q * length, (q + 1) * length), slice(h * HEAD_DIM, (h + 1) * HEAD_DIM))
        for q in range(sequences)
        for h in range(tile // HEAD_DIM)
    ]
    scores = [
        lax.dot_general(query[c], keys[c], (((1,), (1,)), ((), ())), preferred_element_type=F32)
        for c in spans
    ]
    scores = [jnp.where(causal, s * (HEAD_DIM**-0.5), -jnp.inf) for s in scores]
    weights = [jnp.exp(s - jnp.max(s, axis=-1, keepdims=True)) for s in scores]
    probs = [(w / jnp.sum(w, axis=-1, keepdims=True)).astype(BF) for w in weights]
    for p, c in zip(probs, spans):
        heads[c] = dot(p, values[c]).astype(BF)
    for i in range(blocks):
        dest = lax.rem(part + i, blocks)
        product = dot(heads[...], wo[:, pl.ds(pl.multiple_of(dest * tile, tile), tile)])
        if i == 0:
            ys[i][...] = wide[0] + product
        else:
            ys[i][...] = product.astype(BF)


def layer(length, first, meta, jobs, xs, weights):
    rows, tile = xs[0].shape
    blocks = len(xs)
    vmem = pl.BlockSpec(memory_space=pltpu.VMEM)
    smem = pl.BlockSpec(memory_space=pltpu.SMEM)
    return pl.pallas_call(
        functools.partial(layer_kernel, length, first),
        out_shape=[
            jax.ShapeDtypeStruct((rows, tile), F32 if i == 0 else BF) for i in range(blocks)
        ],
        in_specs=[smem, smem] + [vmem] * (blocks + 7),
        out_specs=[vmem] * blocks,
        scratch_shapes=[
            pltpu.VMEM((blocks, rows, tile), BF),
            pltpu.VMEM((rows, tile), BF),
        ],
        cost_estimate=pl.CostEstimate(
            flops=4 * 10**9, bytes_accessed=8 * tile * tile * blocks, transcendentals=0
        ),
        compiler_params=pltpu.CompilerParams(vmem_limit_bytes=8 * 1024 * 1024),
        name="layer",
    )(meta, jobs, *xs, *weights)


def shards(
    inputs,
    sequence_jobs,
    entry_sequence,
    layer_norm_gain,
    frozen_query_matrix,
    frozen_key_matrix,
    frozen_value_matrix,
    frozen_output_matrix,
    adapter_down_maps,
    adapter_up_maps,
):
    sections = lax.axis_size("section")
    across = lax.axis_size("tensor")
    stages = sections // 2
    section_id = lax.axis_index("section")
    part = lax.axis_index("tensor")
    core = section_id % 2
    stage = section_id // 2
    batches, _, length, piece = inputs.shape
    tile = frozen_query_matrix.shape[2]
    streams = 2
    both = ("section", "tensor")

    def turned(value, step):
        return lax.ppermute(
            value, "tensor", [(i, (i + step) % across) for i in range(across)]
        )

    def swapped(value):
        return lax.ppermute(value, "section", [(i, i ^ 1) for i in range(sections)])

    def onward(value):
        return lax.ppermute(value, "section", [(i, i + 2) for i in range(sections - 2)])

    def tokens(which):
        return jnp.concatenate(
            [
                lax.dynamic_slice(
                    inputs, (entry_sequence[m], which, 0, 0), (1, 1, length, piece)
                ).reshape(1, length, piece)
                for m in range(batches)
            ],
            axis=0,
        )

    traded = jnp.stack([tokens(core), swapped(tokens(1 - core))])
    entering = assemble(
        core.reshape(1).astype(jnp.int32),
        [
            lax.ppermute(
                traded,
                both,
                [
                    ((2 * j + e) * across + r, e * across + j)
                    for j in range(stages)
                    for e in range(2)
                ],
            )
            for r in range(across)
        ],
    )

    down_own = adapter_down_maps[0]
    down_all = jnp.stack([down_own] + [turned(down_own, d) for d in range(1, across)])
    own = (
        frozen_query_matrix[0],
        frozen_key_matrix[0],
        frozen_value_matrix[0],
        frozen_output_matrix[0],
        down_all,
        adapter_up_maps[0],
        layer_norm_gain.reshape(across, 1, tile),
    )
    other = tuple(swapped(w) for w in own)
    weights = [
        load(c.reshape(1).astype(jnp.int32), own, other, limit)
        for c, limit in ((core, 44), (1 - core, 32))
    ]
    meta = part.reshape(1).astype(jnp.int32)
    jobs = lax.dynamic_index_in_dim(sequence_jobs[:, :, 0], core, 1, keepdims=False)[entry_sequence]

    def gathered(x):
        return [x] + [turned(x, d) for d in range(1, across)]

    def scattered(ys):
        total = ys[0]
        for d in range(1, across):
            total = total + turned(ys[d], d).astype(F32)
        return total.astype(BF)

    def spread(block):
        first, second = block[..., : tile // 2], block[..., tile // 2 :]
        same = jnp.where(core == 0, first, second)
        cross = jnp.where(core == 0, second, first)
        total = None
        for r in range(across):
            c = slice(r * piece, (r + 1) * piece)
            got = lax.ppermute(
                jnp.stack([same[..., c], cross[..., c]]),
                both,
                [
                    ((sections - 2 + e) * across + j, (2 * j + e) * across + r)
                    for j in range(stages)
                    for e in range(2)
                ],
            )
            total = got if total is None else total + got
        mine, theirs = total[0], swapped(total[1])
        return jnp.where(
            core == 0, jnp.stack([mine, theirs], axis=1), jnp.stack([theirs, mine], axis=1)
        )

    group = batches // streams
    xs = [
        entering[s * group : (s + 1) * group].reshape(group * length, tile) for s in range(streams)
    ]
    for step in range(stages):
        for w in weights:
            for s in range(streams):
                xs[s] = scattered(layer(length, s * group, meta, jobs, gathered(xs[s]), w))
        if step < stages - 1:
            xs = [onward(x) for x in xs]
    return jnp.concatenate([spread(x.reshape(group, length, tile)) for x in xs], axis=0)


def solution(mesh):
    in_specs = (
        P("dp", None, None, ("section", "tensor")),
        P("dp", None, None),
        P("dp"),
        P("section", None),
        P("section", None, "tensor"),
        P("section", None, "tensor"),
        P("section", None, "tensor"),
        P("section", "tensor", None),
        P("section", "tensor", None),
        P("section", None, None, "tensor"),
    )
    out_specs = P("dp", None, None, ("section", "tensor"))
    return jax.shard_map(shards, mesh=mesh, in_specs=in_specs, out_specs=out_specs, check_vma=False)
```

```python
import functools

import jax
import jax.numpy as jnp
from jax import lax
from jax.experimental import pallas as pl
from jax.experimental.pallas import tpu as pltpu
from jax.sharding import PartitionSpec as P

HEAD_DIM = 128
ADAPTER_RANK = 16
ADAPTER_JOBS = 4
SCALE = 2.0
EPS = 1e-05
BF = jnp.bfloat16
F32 = jnp.float32


def dot(a, b):
    return jnp.dot(a, b, preferred_element_type=F32)


def core_of_chip():
    return lax.rem(lax.axis_index("section"), 2)


def load_kernel(layer_of_chip, *refs):
    count = (len(refs) - 1) // 3
    own, other, out, sems = refs[:count], refs[count : 2 * count], refs[2 * count : -1], refs[-1]

    def start(source):
        for n in range(count):
            pltpu.make_async_copy(source[n], out[n], sems.at[n]).start()

    mine = core_of_chip() == layer_of_chip

    @pl.when(mine)
    def _():
        start(own)

    @pl.when(jnp.logical_not(mine))
    def _():
        start(other)

    for n in range(count):
        pltpu.make_async_copy(own[n], out[n], sems.at[n]).wait()


def load(layer_of_chip, own, other):
    vmem = pl.BlockSpec(memory_space=pltpu.VMEM)
    hbm = pl.BlockSpec(memory_space=pltpu.HBM)
    count = len(own)
    return pl.pallas_call(
        functools.partial(load_kernel, layer_of_chip),
        out_shape=[jax.ShapeDtypeStruct(w.shape, w.dtype) for w in own],
        in_specs=[hbm] * (2 * count),
        out_specs=[vmem] * count,
        scratch_shapes=[pltpu.SemaphoreType.DMA((count,))],
        cost_estimate=pl.CostEstimate(
            flops=4 * 10**9, bytes_accessed=8 * own[0].size, transcendentals=0
        ),
        compiler_params=pltpu.CompilerParams(vmem_limit_bytes=2 * 1024 * 1024),
        name="load",
    )(*own, *other)


def pick_kernel(entry, tokens, mine, theirs):
    core = core_of_chip()
    for m in range(tokens.shape[0]):
        mine[m] = tokens[entry[m], core]
        theirs[m] = tokens[entry[m], 1 - core]


def assemble_kernel(after, *refs):
    del after
    pieces, out = refs[:-1], refs[-1]
    count = len(pieces)
    width = pieces[0].shape[3]
    first = core_of_chip() == 0
    for r, piece in enumerate(pieces):
        same, cross = piece[0], piece[1]
        out[:, :, r * width : (r + 1) * width] = jnp.where(first, same, cross)
        out[:, :, (count + r) * width : (count + r + 1) * width] = jnp.where(first, cross, same)


def split_kernel(block, *pieces):
    count = len(pieces)
    _, sequences, length, width = pieces[0].shape
    first = core_of_chip() == 0
    for q in range(sequences):
        rows = slice(q * length, (q + 1) * length)
        for r, piece in enumerate(pieces):
            low = block[rows, r * width : (r + 1) * width]
            high = block[rows, (count + r) * width : (count + r + 1) * width]
            piece[0, q] = jnp.where(first, low, high)
            piece[1, q] = jnp.where(first, high, low)


def merge_kernel(*refs):
    streams = (len(refs) - 1) // 2
    out = refs[-1]
    first = core_of_chip() == 0
    for s in range(streams):
        mine, theirs = refs[s][...], refs[streams + s][...]
        span = slice(s * mine.shape[0], (s + 1) * mine.shape[0])
        out[span, 0] = jnp.where(first, mine, theirs)
        out[span, 1] = jnp.where(first, theirs, mine)


def call(kernel, name, shapes, inputs, smem=0):
    vmem = pl.BlockSpec(memory_space=pltpu.VMEM)
    return pl.pallas_call(
        kernel,
        out_shape=[jax.ShapeDtypeStruct(s, BF) for s in shapes],
        in_specs=[pl.BlockSpec(memory_space=pltpu.SMEM)] * smem + [vmem] * (len(inputs) - smem),
        out_specs=[vmem] * len(shapes),
        compiler_params=pltpu.CompilerParams(vmem_limit_bytes=8 * 1024 * 1024),
        name=name,
    )(*inputs)


def layer_kernel(
    length, first, entry, jobs, x0, x1, x2, x3, wq, wk, wv, wo, down, up, gain, y0, y1, y2, y3, normed, heads
):
    xs, ys = (x0, x1, x2, x3), (y0, y1, y2, y3)
    rows, tile = x0.shape
    blocks = len(xs)
    part = lax.axis_index("tensor")
    core = core_of_chip()
    sequences = rows // length
    column_job = (
        lax.broadcasted_iota(jnp.int32, (length, down.shape[2]), 1) // ADAPTER_RANK % ADAPTER_JOBS
    )
    own_job = jnp.concatenate(
        [(column_job == jobs[entry[first + q], core]).astype(F32) for q in range(sequences)], axis=0
    )
    wide = [x[...].astype(F32) for x in xs]
    square = sum(jnp.sum(w * w, axis=-1, keepdims=True) for w in wide)
    norm = lax.rsqrt(square * (1.0 / (tile * blocks)) + EPS)
    codes = None
    for i in range(blocks):
        rank = lax.rem(part + (blocks - i), blocks)
        block = (wide[i] * norm * gain[rank]).astype(BF)
        normed[rank] = block
        code = dot(block, down[i])
        codes = code if codes is None else codes + code
    codes = jnp.where(own_job > 0.0, codes, 0.0).astype(BF)
    half = codes.shape[1] // 2

    def projected(w):
        total = None
        for i in range(blocks):
            product = dot(normed[i], w[i * tile : (i + 1) * tile])
            total = product if total is None else total + product
        return total

    query = (projected(wq) + SCALE * dot(codes[:, :half], up[0])).astype(BF)
    keys = projected(wk).astype(BF)
    values = (projected(wv) + SCALE * dot(codes[:, half:], up[1])).astype(BF)
    causal = lax.broadcasted_iota(jnp.int32, (length, length), 0) >= lax.broadcasted_iota(
        jnp.int32, (length, length), 1
    )
    spans = [
        (slice(q * length, (q + 1) * length), slice(h * HEAD_DIM, (h + 1) * HEAD_DIM))
        for q in range(sequences)
        for h in range(tile // HEAD_DIM)
    ]
    scores = [
        lax.dot_general(query[c], keys[c], (((1,), (1,)), ((), ())), preferred_element_type=F32)
        for c in spans
    ]
    scores = [jnp.where(causal, s * (HEAD_DIM**-0.5), -jnp.inf) for s in scores]
    weights = [jnp.exp(s - jnp.max(s, axis=-1, keepdims=True)) for s in scores]
    probs = [(w / jnp.sum(w, axis=-1, keepdims=True)).astype(BF) for w in weights]
    for p, c in zip(probs, spans):
        heads[c] = dot(p, values[c]).astype(BF)
    for i in range(blocks):
        dest = lax.rem(part + i, blocks)
        product = dot(heads[...], wo[:, pl.ds(pl.multiple_of(dest * tile, tile), tile)])
        if i == 0:
            ys[i][...] = wide[0] + product
        else:
            ys[i][...] = product.astype(BF)


def layer(length, first, entry, jobs, xs, weights):
    rows, tile = xs[0].shape
    blocks = len(xs)
    vmem = pl.BlockSpec(memory_space=pltpu.VMEM)
    smem = pl.BlockSpec(memory_space=pltpu.SMEM)
    return pl.pallas_call(
        functools.partial(layer_kernel, length, first),
        out_shape=[
            jax.ShapeDtypeStruct((rows, tile), F32 if i == 0 else BF) for i in range(blocks)
        ],
        in_specs=[smem, smem] + [vmem] * (blocks + 7),
        out_specs=[vmem] * blocks,
        scratch_shapes=[
            pltpu.VMEM((blocks, rows, tile), BF),
            pltpu.VMEM((rows, tile), BF),
        ],
        cost_estimate=pl.CostEstimate(
            flops=4 * 10**9, bytes_accessed=8 * tile * tile * blocks, transcendentals=0
        ),
        compiler_params=pltpu.CompilerParams(vmem_limit_bytes=8 * 1024 * 1024),
        name="layer",
    )(entry, jobs, *xs, *weights)


def shards(
    inputs,
    sequence_jobs,
    entry_sequence,
    layer_norm_gain,
    frozen_query_matrix,
    frozen_key_matrix,
    frozen_value_matrix,
    frozen_output_matrix,
    adapter_down_maps,
    adapter_up_maps,
):
    sections = lax.axis_size("section")
    across = lax.axis_size("tensor")
    stages = sections // 2
    batches, _, length, piece = inputs.shape
    tile = frozen_query_matrix.shape[2]
    streams = 2
    both = ("section", "tensor")

    def turned(value, step):
        return lax.ppermute(
            value, "tensor", [(i, (i + step) % across) for i in range(across)]
        )

    def swapped(value):
        return lax.ppermute(value, "section", [(i, i ^ 1) for i in range(sections)])

    def onward(value):
        return lax.ppermute(value, "section", [(i, i + 2) for i in range(sections - 2)])

    down_own = adapter_down_maps[0]
    down_all = jnp.stack([down_own] + [turned(down_own, d) for d in range(1, across)])
    own = (
        frozen_query_matrix[0],
        frozen_key_matrix[0],
        frozen_value_matrix[0],
        frozen_output_matrix[0],
        down_all,
        adapter_up_maps[0],
        layer_norm_gain.reshape(across, 1, tile),
    )
    other = tuple(swapped(w) for w in own)
    weights = [load(l, own, other) for l in range(2)]
    jobs = sequence_jobs[:, :, 0]

    shape = (batches, length, piece)
    mine, theirs = call(pick_kernel, "pick", [shape] * 2, [entry_sequence, inputs], smem=1)
    traded = jnp.stack([mine, swapped(theirs)])
    pieces = [
        lax.ppermute(
            traded,
            both,
            [
                ((2 * j + e) * across + r, e * across + j)
                for j in range(stages)
                for e in range(2)
            ],
        )
        for r in range(across)
    ]
    (entering,) = call(
        assemble_kernel, "assemble", [(batches, length, tile)], [weights[0][6]] + pieces
    )

    def gathered(x):
        return [x] + [turned(x, d) for d in range(1, across)]

    def scattered(ys):
        total = ys[0]
        for d in range(1, across):
            total = total + turned(ys[d], d).astype(F32)
        return total.astype(BF)

    group = batches // streams

    def spread(block):
        parts = call(split_kernel, "split", [(2, group, length, piece)] * across, [block])
        total = None
        for r in range(across):
            got = lax.ppermute(
                parts[r],
                both,
                [
                    ((sections - 2 + e) * across + j, (2 * j + e) * across + r)
                    for j in range(stages)
                    for e in range(2)
                ],
            )
            total = got if total is None else total + got
        return total[0], swapped(total[1])

    xs = [
        entering[s * group : (s + 1) * group].reshape(group * length, tile) for s in range(streams)
    ]
    for step in range(stages):
        for w in weights:
            for s in range(streams):
                ys = layer(length, s * group, entry_sequence, jobs, gathered(xs[s]), w)
                xs[s] = scattered(ys)
        if step < stages - 1:
            xs = [onward(x) for x in xs]
    found = [spread(x) for x in xs]
    (finished,) = call(
        merge_kernel,
        "merge",
        [(batches, 2, length, piece)],
        [f[0] for f in found] + [f[1] for f in found],
    )
    return finished


def solution(mesh):
    in_specs = (
        P("dp", None, None, ("section", "tensor")),
        P("dp", None, None),
        P("dp"),
        P("section", None),
        P("section", None, "tensor"),
        P("section", None, "tensor"),
        P("section", None, "tensor"),
        P("section", "tensor", None),
        P("section", "tensor", None),
        P("section", None, None, "tensor"),
    )
    out_specs = P("dp", None, None, ("section", "tensor"))
    return jax.shard_map(shards, mesh=mesh, in_specs=in_specs, out_specs=out_specs, check_vma=False)
```

```python
import functools

import jax
import jax.numpy as jnp
from jax import lax
from jax.experimental import pallas as pl
from jax.experimental.pallas import tpu as pltpu
from jax.sharding import PartitionSpec as P

HEAD_DIM = 128
ADAPTER_RANK = 16
ADAPTER_JOBS = 4
SCALE = 2.0
EPS = 1e-05
N_TENSOR = 4
BF = jnp.bfloat16
F32 = jnp.float32


def dot(a, b):
    return jnp.dot(a, b, preferred_element_type=F32)


def core_of_chip():
    return lax.rem(lax.axis_index("section"), 2)


def load_kernel(*refs):
    count, outs = 6 + N_TENSOR, 7
    own, other = refs[:count], refs[count : 2 * count]
    out, sems = refs[2 * count : -1], refs[-1]
    target = [
        [*out[l * outs : l * outs + 6], *(out[l * outs + 6].at[i] for i in range(N_TENSOR))]
        for l in range(2)
    ]

    def start(sources):
        for l in range(2):
            for n in range(count):
                pltpu.make_async_copy(sources[l][n], target[l][n], sems.at[l, n]).start()

    core = core_of_chip()

    @pl.when(core == 0)
    def _():
        start((own, other))

    @pl.when(core != 0)
    def _():
        start((other, own))

    for l in range(2):
        for n in range(count):
            pltpu.make_async_copy(own[n], target[l][n], sems.at[l, n]).wait()


def load(own, other):
    vmem = pl.BlockSpec(memory_space=pltpu.VMEM)
    hbm = pl.BlockSpec(memory_space=pltpu.HBM)
    count = len(own)
    shapes = [w.shape for w in own[:6]] + [(N_TENSOR, *own[6].shape)]
    types = [w.dtype for w in own[:6]] + [BF]
    found = pl.pallas_call(
        load_kernel,
        out_shape=[jax.ShapeDtypeStruct(s, t) for s, t in zip(shapes * 2, types * 2)],
        in_specs=[hbm] * (2 * count),
        out_specs=[vmem] * (2 * len(shapes)),
        scratch_shapes=[pltpu.SemaphoreType.DMA((2, count))],
        cost_estimate=pl.CostEstimate(
            flops=4 * 10**9, bytes_accessed=16 * own[0].size, transcendentals=0
        ),
        compiler_params=pltpu.CompilerParams(vmem_limit_bytes=33 * 1024 * 1024),
        name="load",
    )(*own, *other)
    return found[: len(shapes)], found[len(shapes) :]


def pick_kernel(entry, owners, tokens, mine, theirs, jobs):
    core = core_of_chip()
    for m in range(tokens.shape[0]):
        jobs[m] = owners[entry[m], core, 0]
        mine[m] = tokens[entry[m], core]
        theirs[m] = tokens[entry[m], 1 - core]


def assemble_kernel(after, *refs):
    del after
    pieces, out = refs[:-1], refs[-1]
    count = len(pieces)
    width = pieces[0].shape[3]
    first = core_of_chip() == 0
    for r, piece in enumerate(pieces):
        same, cross = piece[0], piece[1]
        out[:, :, r * width : (r + 1) * width] = jnp.where(first, same, cross)
        out[:, :, (count + r) * width : (count + r + 1) * width] = jnp.where(first, cross, same)


def split_kernel(block, *pieces):
    count = len(pieces)
    _, sequences, length, width = pieces[0].shape
    first = core_of_chip() == 0
    for q in range(sequences):
        rows = slice(q * length, (q + 1) * length)
        for r, piece in enumerate(pieces):
            low = block[rows, r * width : (r + 1) * width]
            high = block[rows, (count + r) * width : (count + r + 1) * width]
            piece[0, q] = jnp.where(first, low, high)
            piece[1, q] = jnp.where(first, high, low)


def merge_kernel(*refs):
    streams = (len(refs) - 1) // 2
    out = refs[-1]
    first = core_of_chip() == 0
    for s in range(streams):
        mine, theirs = refs[s][...], refs[streams + s][...]
        span = slice(s * mine.shape[0], (s + 1) * mine.shape[0])
        out[span, 0] = jnp.where(first, mine, theirs)
        out[span, 1] = jnp.where(first, theirs, mine)


def call(kernel, name, shapes, inputs):
    vmem = pl.BlockSpec(memory_space=pltpu.VMEM)
    return pl.pallas_call(
        kernel,
        out_shape=[jax.ShapeDtypeStruct(s, BF) for s in shapes],
        in_specs=[vmem] * len(inputs),
        out_specs=[vmem] * len(shapes),
        compiler_params=pltpu.CompilerParams(vmem_limit_bytes=2 * 1024 * 1024),
        name=name,
    )(*inputs)


def layer_kernel(
    length, first, jobs, x0, x1, x2, x3, wq, wk, wv, wo, up, gain, down, y0, y1, y2, y3, normed, heads
):
    xs, ys = (x0, x1, x2, x3), (y0, y1, y2, y3)
    rows, tile = x0.shape
    blocks = len(xs)
    part = lax.axis_index("tensor")
    sequences = rows // length
    column_job = (
        lax.broadcasted_iota(jnp.int32, (length, down.shape[2]), 1) // ADAPTER_RANK % ADAPTER_JOBS
    )
    own_job = jnp.concatenate(
        [(column_job == jobs[first + q]).astype(F32) for q in range(sequences)], axis=0
    )
    wide = [x[...].astype(F32) for x in xs]
    square = sum(jnp.sum(w * w, axis=-1, keepdims=True) for w in wide)
    norm = lax.rsqrt(square * (1.0 / (tile * blocks)) + EPS)
    codes = None
    for i in range(blocks):
        rank = lax.rem(part + (blocks - i), blocks)
        block = (wide[i] * norm * gain[rank]).astype(BF)
        normed[rank] = block
        code = dot(block, down[i])
        codes = code if codes is None else codes + code
    codes = jnp.where(own_job > 0.0, codes, 0.0).astype(BF)
    half = codes.shape[1] // 2

    def projected(w):
        total = None
        for i in range(blocks):
            product = dot(normed[i], w[i * tile : (i + 1) * tile])
            total = product if total is None else total + product
        return total

    query = (projected(wq) + SCALE * dot(codes[:, :half], up[0])).astype(BF)
    keys = projected(wk).astype(BF)
    values = (projected(wv) + SCALE * dot(codes[:, half:], up[1])).astype(BF)
    causal = lax.broadcasted_iota(jnp.int32, (length, length), 0) >= lax.broadcasted_iota(
        jnp.int32, (length, length), 1
    )
    spans = [
        (slice(q * length, (q + 1) * length), slice(h * HEAD_DIM, (h + 1) * HEAD_DIM))
        for q in range(sequences)
        for h in range(tile // HEAD_DIM)
    ]
    scores = [
        lax.dot_general(query[c], keys[c], (((1,), (1,)), ((), ())), preferred_element_type=F32)
        for c in spans
    ]
    scores = [jnp.where(causal, s * (HEAD_DIM**-0.5), -jnp.inf) for s in scores]
    weights = [jnp.exp(s - jnp.max(s, axis=-1, keepdims=True)) for s in scores]
    probs = [(w / jnp.sum(w, axis=-1, keepdims=True)).astype(BF) for w in weights]
    for p, c in zip(probs, spans):
        heads[c] = dot(p, values[c]).astype(BF)
    for i in range(blocks):
        dest = lax.rem(part + i, blocks)
        product = dot(heads[...], wo[:, pl.ds(pl.multiple_of(dest * tile, tile), tile)])
        if i == 0:
            ys[i][...] = wide[0] + product
        else:
            ys[i][...] = product.astype(BF)


def layer(length, first, jobs, xs, weights):
    rows, tile = xs[0].shape
    blocks = len(xs)
    vmem = pl.BlockSpec(memory_space=pltpu.VMEM)
    smem = pl.BlockSpec(memory_space=pltpu.SMEM)
    return pl.pallas_call(
        functools.partial(layer_kernel, length, first),
        out_shape=[
            jax.ShapeDtypeStruct((rows, tile), F32 if i == 0 else BF) for i in range(blocks)
        ],
        in_specs=[smem] + [vmem] * (blocks + 7),
        out_specs=[vmem] * blocks,
        scratch_shapes=[
            pltpu.VMEM((blocks, rows, tile), BF),
            pltpu.VMEM((rows, tile), BF),
        ],
        cost_estimate=pl.CostEstimate(
            flops=4 * 10**9, bytes_accessed=8 * tile * tile * blocks, transcendentals=0
        ),
        compiler_params=pltpu.CompilerParams(vmem_limit_bytes=8 * 1024 * 1024),
        name="layer",
    )(jobs, *xs, *weights)


def shards(
    inputs,
    sequence_jobs,
    entry_sequence,
    layer_norm_gain,
    frozen_query_matrix,
    frozen_key_matrix,
    frozen_value_matrix,
    frozen_output_matrix,
    adapter_down_maps,
    adapter_up_maps,
):
    sections = lax.axis_size("section")
    across = lax.axis_size("tensor")
    stages = sections // 2
    batches, _, length, piece = inputs.shape
    tile = frozen_query_matrix.shape[2]
    streams = 2
    both = ("section", "tensor")

    def turned(value, step):
        return lax.ppermute(
            value, "tensor", [(i, (i + step) % across) for i in range(across)]
        )

    def swapped(value):
        return lax.ppermute(value, "section", [(i, i ^ 1) for i in range(sections)])

    def onward(value, step):
        return lax.ppermute(value, "section", [(2 * step + e, 2 * step + 2 + e) for e in range(2)])

    shape = (batches, length, piece)
    smem = pl.BlockSpec(memory_space=pltpu.SMEM)
    vmem = pl.BlockSpec(memory_space=pltpu.VMEM)
    mine, theirs, jobs = pl.pallas_call(
        pick_kernel,
        out_shape=[jax.ShapeDtypeStruct(shape, BF)] * 2
        + [jax.ShapeDtypeStruct((batches,), jnp.int32)],
        in_specs=[smem, smem, vmem],
        out_specs=[vmem, vmem, smem],
        compiler_params=pltpu.CompilerParams(vmem_limit_bytes=2 * 1024 * 1024),
        name="pick",
    )(entry_sequence, sequence_jobs, inputs)
    down_own, mine, theirs = lax.optimization_barrier((adapter_down_maps[0], mine, theirs))
    downs = [down_own] + [turned(down_own, d) for d in range(1, across)]
    own = (
        frozen_query_matrix[0],
        frozen_key_matrix[0],
        frozen_value_matrix[0],
        frozen_output_matrix[0],
        adapter_up_maps[0],
        layer_norm_gain.reshape(across, 1, tile),
        *downs,
    )
    other = tuple(swapped(w) for w in own)
    weights = load(own, other)
    traded = jnp.stack([mine, swapped(theirs)])
    pieces = [
        lax.ppermute(
            traded,
            both,
            [
                ((2 * j + e) * across + r, e * across + j)
                for j in range(stages)
                for e in range(2)
            ],
        )
        for r in range(across)
    ]
    (entering,) = call(
        assemble_kernel, "assemble", [(batches, length, tile)], [weights[0][5]] + pieces
    )

    def gathered(x):
        return [x] + [turned(x, d) for d in range(1, across)]

    def scattered(ys):
        total = ys[0]
        for d in range(1, across):
            total = total + turned(ys[d], d).astype(F32)
        return total.astype(BF)

    group = batches // streams

    def spread(block):
        parts = call(split_kernel, "split", [(2, group, length, piece)] * across, [block])
        total = None
        for r in range(across):
            got = lax.ppermute(
                parts[r],
                both,
                [
                    ((sections - 2 + e) * across + j, (2 * j + e) * across + r)
                    for j in range(stages)
                    for e in range(2)
                ],
            )
            total = got if total is None else total + got
        return total[0], swapped(total[1])

    xs = [
        entering[s * group : (s + 1) * group].reshape(group * length, tile) for s in range(streams)
    ]
    for step in range(stages):
        for w in weights:
            for s in range(streams):
                ys = layer(length, s * group, jobs, gathered(xs[s]), w)
                xs[s] = scattered(ys)
        if step < stages - 1:
            xs = [onward(x, step) for x in xs]
    found = [spread(x) for x in xs]
    (finished,) = call(
        merge_kernel,
        "merge",
        [(batches, 2, length, piece)],
        [f[0] for f in found] + [f[1] for f in found],
    )
    return finished


def solution(mesh):
    in_specs = (
        P("dp", None, None, ("section", "tensor")),
        P("dp", None, None),
        P("dp"),
        P("section", None),
        P("section", None, "tensor"),
        P("section", None, "tensor"),
        P("section", None, "tensor"),
        P("section", "tensor", None),
        P("section", "tensor", None),
        P("section", None, None, "tensor"),
    )
    out_specs = P("dp", None, None, ("section", "tensor"))
    return jax.shard_map(shards, mesh=mesh, in_specs=in_specs, out_specs=out_specs, check_vma=False)
```

```python
import functools

import jax
import jax.numpy as jnp
from jax import lax
from jax.experimental import pallas as pl
from jax.experimental.pallas import tpu as pltpu
from jax.sharding import PartitionSpec as P

HEAD_DIM = 128
ADAPTER_RANK = 16
ADAPTER_JOBS = 4
SCALE = 2.0
EPS = 1e-05
N_TENSOR = 4
BF = jnp.bfloat16
F32 = jnp.float32


def dot(a, b):
    return jnp.dot(a, b, preferred_element_type=F32)


def core_of_chip():
    return lax.rem(lax.axis_index("section"), 2)


def load_kernel(*refs):
    count, outs = 6 + N_TENSOR, 7
    own, other = refs[:count], refs[count : 2 * count]
    out, sems = refs[2 * count : -1], refs[-1]
    target = [
        [*out[l * outs : l * outs + 6], *(out[l * outs + 6].at[i] for i in range(N_TENSOR))]
        for l in range(2)
    ]

    def start(sources):
        for l in range(2):
            for n in range(count):
                pltpu.make_async_copy(sources[l][n], target[l][n], sems.at[l, n]).start()

    core = core_of_chip()

    @pl.when(core == 0)
    def _():
        start((own, other))

    @pl.when(core != 0)
    def _():
        start((other, own))

    for l in range(2):
        for n in range(count):
            pltpu.make_async_copy(own[n], target[l][n], sems.at[l, n]).wait()


def load(own, other):
    vmem = pl.BlockSpec(memory_space=pltpu.VMEM)
    hbm = pl.BlockSpec(memory_space=pltpu.HBM)
    count = len(own)
    shapes = [w.shape for w in own[:6]] + [(N_TENSOR, *own[6].shape)]
    types = [w.dtype for w in own[:6]] + [BF]
    found = pl.pallas_call(
        load_kernel,
        out_shape=[jax.ShapeDtypeStruct(s, t) for s, t in zip(shapes * 2, types * 2)],
        in_specs=[hbm] * (2 * count),
        out_specs=[vmem] * (2 * len(shapes)),
        scratch_shapes=[pltpu.SemaphoreType.DMA((2, count))],
        cost_estimate=pl.CostEstimate(
            flops=4 * 10**9, bytes_accessed=16 * own[0].size, transcendentals=0
        ),
        compiler_params=pltpu.CompilerParams(vmem_limit_bytes=33 * 1024 * 1024),
        name="load",
    )(*own, *other)
    return found[: len(shapes)], found[len(shapes) :]


def pick_kernel(entry, owners, tokens, mine, theirs, jobs):
    core = core_of_chip()
    for m in range(tokens.shape[0]):
        jobs[m] = owners[entry[m], core, 0]
        mine[m] = tokens[entry[m], core]
        theirs[m] = tokens[entry[m], 1 - core]


def assemble_kernel(*refs):
    pieces, out = refs[:-1], refs[-1]
    count = len(pieces)
    width = pieces[0].shape[3]
    first = core_of_chip() == 0
    for r, piece in enumerate(pieces):
        same, cross = piece[0], piece[1]
        out[:, :, r * width : (r + 1) * width] = jnp.where(first, same, cross)
        out[:, :, (count + r) * width : (count + r + 1) * width] = jnp.where(first, cross, same)


def split_kernel(block, *pieces):
    count = len(pieces)
    _, sequences, length, width = pieces[0].shape
    first = core_of_chip() == 0
    for q in range(sequences):
        rows = slice(q * length, (q + 1) * length)
        for r, piece in enumerate(pieces):
            low = block[rows, r * width : (r + 1) * width]
            high = block[rows, (count + r) * width : (count + r + 1) * width]
            piece[0, q] = jnp.where(first, low, high)
            piece[1, q] = jnp.where(first, high, low)


def merge_kernel(*refs):
    streams = (len(refs) - 1) // 2
    out = refs[-1]
    first = core_of_chip() == 0
    for s in range(streams):
        mine, theirs = refs[s][...], refs[streams + s][...]
        span = slice(s * mine.shape[0], (s + 1) * mine.shape[0])
        out[span, 0] = jnp.where(first, mine, theirs)
        out[span, 1] = jnp.where(first, theirs, mine)


def call(kernel, name, shapes, inputs):
    vmem = pl.BlockSpec(memory_space=pltpu.VMEM)
    return pl.pallas_call(
        kernel,
        out_shape=[jax.ShapeDtypeStruct(s, BF) for s in shapes],
        in_specs=[vmem] * len(inputs),
        out_specs=[vmem] * len(shapes),
        compiler_params=pltpu.CompilerParams(vmem_limit_bytes=2 * 1024 * 1024),
        name=name,
    )(*inputs)


def layer_kernel(
    length, first, jobs, x0, x1, x2, x3, wq, wk, wv, wo, up, gain, down, y0, y1, y2, y3, normed, heads
):
    xs, ys = (x0, x1, x2, x3), (y0, y1, y2, y3)
    rows, tile = x0.shape
    blocks = len(xs)
    part = lax.axis_index("tensor")
    sequences = rows // length
    column_job = (
        lax.broadcasted_iota(jnp.int32, (length, down.shape[2]), 1) // ADAPTER_RANK % ADAPTER_JOBS
    )
    own_job = jnp.concatenate(
        [(column_job == jobs[first + q]).astype(F32) for q in range(sequences)], axis=0
    )
    wide = [x[...].astype(F32) for x in xs]
    square = sum(jnp.sum(w * w, axis=-1, keepdims=True) for w in wide)
    norm = lax.rsqrt(square * (1.0 / (tile * blocks)) + EPS)
    codes = None
    for i in range(blocks):
        rank = lax.rem(part + (blocks - i), blocks)
        block = (wide[i] * norm * gain[rank]).astype(BF)
        normed[rank] = block
        code = dot(block, down[i])
        codes = code if codes is None else codes + code
    codes = jnp.where(own_job > 0.0, codes, 0.0).astype(BF)
    half = codes.shape[1] // 2

    def projected(w):
        total = None
        for i in range(blocks):
            product = dot(normed[i], w[i * tile : (i + 1) * tile])
            total = product if total is None else total + product
        return total

    query = (projected(wq) + SCALE * dot(codes[:, :half], up[0])).astype(BF)
    keys = projected(wk).astype(BF)
    values = (projected(wv) + SCALE * dot(codes[:, half:], up[1])).astype(BF)
    causal = lax.broadcasted_iota(jnp.int32, (length, length), 0) >= lax.broadcasted_iota(
        jnp.int32, (length, length), 1
    )
    spans = [
        (slice(q * length, (q + 1) * length), slice(h * HEAD_DIM, (h + 1) * HEAD_DIM))
        for q in range(sequences)
        for h in range(tile // HEAD_DIM)
    ]
    scores = [
        lax.dot_general(query[c], keys[c], (((1,), (1,)), ((), ())), preferred_element_type=F32)
        for c in spans
    ]
    scores = [jnp.where(causal, s * (HEAD_DIM**-0.5), -jnp.inf) for s in scores]
    weights = [jnp.exp(s - jnp.max(s, axis=-1, keepdims=True)) for s in scores]
    probs = [(w / jnp.sum(w, axis=-1, keepdims=True)).astype(BF) for w in weights]
    for p, c in zip(probs, spans):
        heads[c] = dot(p, values[c]).astype(BF)
    for i in range(blocks):
        dest = lax.rem(part + i, blocks)
        product = dot(heads[...], wo[:, pl.ds(pl.multiple_of(dest * tile, tile), tile)])
        if i == 0:
            ys[i][...] = wide[0] + product
        else:
            ys[i][...] = product.astype(BF)


def layer(length, first, jobs, xs, weights):
    rows, tile = xs[0].shape
    blocks = len(xs)
    vmem = pl.BlockSpec(memory_space=pltpu.VMEM)
    smem = pl.BlockSpec(memory_space=pltpu.SMEM)
    return pl.pallas_call(
        functools.partial(layer_kernel, length, first),
        out_shape=[
            jax.ShapeDtypeStruct((rows, tile), F32 if i == 0 else BF) for i in range(blocks)
        ],
        in_specs=[smem] + [vmem] * (blocks + 7),
        out_specs=[vmem] * blocks,
        scratch_shapes=[
            pltpu.VMEM((blocks, rows, tile), BF),
            pltpu.VMEM((rows, tile), BF),
        ],
        cost_estimate=pl.CostEstimate(
            flops=4 * 10**9, bytes_accessed=8 * tile * tile * blocks, transcendentals=0
        ),
        compiler_params=pltpu.CompilerParams(vmem_limit_bytes=8 * 1024 * 1024),
        name="layer",
    )(jobs, *xs, *weights)


def shards(
    inputs,
    sequence_jobs,
    entry_sequence,
    layer_norm_gain,
    frozen_query_matrix,
    frozen_key_matrix,
    frozen_value_matrix,
    frozen_output_matrix,
    adapter_down_maps,
    adapter_up_maps,
):
    sections = lax.axis_size("section")
    across = lax.axis_size("tensor")
    stages = sections // 2
    batches, _, length, piece = inputs.shape
    tile = frozen_query_matrix.shape[2]
    streams = 2
    both = ("section", "tensor")

    def turned(value, step):
        return lax.ppermute(
            value, "tensor", [(i, (i + step) % across) for i in range(across)]
        )

    def swapped(value):
        return lax.ppermute(value, "section", [(i, i ^ 1) for i in range(sections)])

    def onward(value, step):
        return lax.ppermute(value, "section", [(2 * step + e, 2 * step + 2 + e) for e in range(2)])

    shape = (batches, length, piece)
    smem = pl.BlockSpec(memory_space=pltpu.SMEM)
    vmem = pl.BlockSpec(memory_space=pltpu.VMEM)
    mine, theirs, jobs = pl.pallas_call(
        pick_kernel,
        out_shape=[jax.ShapeDtypeStruct(shape, BF)] * 2
        + [jax.ShapeDtypeStruct((batches,), jnp.int32)],
        in_specs=[smem, smem, vmem],
        out_specs=[vmem, vmem, smem],
        compiler_params=pltpu.CompilerParams(vmem_limit_bytes=2 * 1024 * 1024),
        name="pick",
    )(entry_sequence, sequence_jobs, inputs)
    traded = jnp.stack([mine, swapped(theirs)])
    down_own, traded = lax.optimization_barrier((adapter_down_maps[0], traded))
    downs = [down_own] + [turned(down_own, d) for d in range(1, across)]
    pieces = [
        lax.ppermute(
            traded,
            both,
            [
                ((2 * j + e) * across + r, e * across + j)
                for j in range(stages)
                for e in range(2)
            ],
        )
        for r in range(across)
    ]
    downs, pieces = lax.optimization_barrier((downs, pieces))
    own = (
        frozen_query_matrix[0],
        frozen_key_matrix[0],
        frozen_value_matrix[0],
        frozen_output_matrix[0],
        adapter_up_maps[0],
        layer_norm_gain.reshape(across, 1, tile),
        *downs,
    )
    other = tuple(swapped(w) for w in own)
    weights = load(own, other)
    (entering,) = call(
        assemble_kernel, "assemble", [(batches, length, tile)], pieces
    )

    def gathered(x):
        return [x] + [turned(x, d) for d in range(1, across)]

    def scattered(ys):
        total = ys[0]
        for d in range(1, across):
            total = total + turned(ys[d], d).astype(F32)
        return total.astype(BF)

    group = batches // streams

    def spread(block):
        parts = call(split_kernel, "split", [(2, group, length, piece)] * across, [block])
        total = None
        for r in range(across):
            got = lax.ppermute(
                parts[r],
                both,
                [
                    ((sections - 2 + e) * across + j, (2 * j + e) * across + r)
                    for j in range(stages)
                    for e in range(2)
                ],
            )
            total = got if total is None else total + got
        return total[0], swapped(total[1])

    xs = [
        entering[s * group : (s + 1) * group].reshape(group * length, tile) for s in range(streams)
    ]
    for step in range(stages):
        for w in weights:
            for s in range(streams):
                ys = layer(length, s * group, jobs, gathered(xs[s]), w)
                xs[s] = scattered(ys)
        if step < stages - 1:
            xs = [onward(x, step) for x in xs]
    found = [spread(x) for x in xs]
    (finished,) = call(
        merge_kernel,
        "merge",
        [(batches, 2, length, piece)],
        [f[0] for f in found] + [f[1] for f in found],
    )
    return finished


def solution(mesh):
    in_specs = (
        P("dp", None, None, ("section", "tensor")),
        P("dp", None, None),
        P("dp"),
        P("section", None),
        P("section", None, "tensor"),
        P("section", None, "tensor"),
        P("section", None, "tensor"),
        P("section", "tensor", None),
        P("section", "tensor", None),
        P("section", None, None, "tensor"),
    )
    out_specs = P("dp", None, None, ("section", "tensor"))
    return jax.shard_map(shards, mesh=mesh, in_specs=in_specs, out_specs=out_specs, check_vma=False)
```
